32 devices in a mesh: gx: 2 (over x), gy: 4 (over z), gz: 4 (over y, core).
Axes of the slice: x: 2, y: 2, z: 4, core: 2. Of those that a mesh axis runs over, the one named last changes fastest.
Arguments:
- fields: float32 [1, 64, 128, 512], P(None, 'gx', 'gy', 'gz'), may hold values from -13 to 13
- exponents: int32 [5], replicated, may hold values from -5 to -1
Outputs:
- coefficients: float32 [1, 64, 128, 512], P(None, 'gx', 'gy', 'gz')
- statistics: float32 [2, 1, 5], replicated
The draws below stay inside these ranges and needn't reach their ends.
All inputs are finite; a program needn't handle non-finite values.
Results may differ from the reference program's by a relative error of at most 0.0003.
Values sent between devices are 32-bit elements; how exact they have to be, the bound alone decides.
A program may use at most 64 MiB of HBM per device.

```python
import jax
import jax.numpy as jnp
from jax import lax

FIELDS = 1
FINE = 3
COARSE = 2
LEVELS = 5
NX = 64
NY = 128
NZ = 512


def coarse_rough(key):
    block = 2 ** FINE
    values = jax.random.uniform(jax.random.fold_in(key, 23), (FIELDS, NX // block, NY // block, NZ // block), jnp.float32, -3.0, 3.0)
    values = jnp.repeat(values, block, axis=1)
    values = jnp.repeat(values, block, axis=2)
    return jnp.repeat(values, block, axis=3)


def draw_fields(key, part):
    shape = (FIELDS, NX, NY, NZ)
    coord_x = jnp.arange(NX, dtype=jnp.float32)[None, :, None, None] / NX
    coord_y = jnp.arange(NY, dtype=jnp.float32)[None, None, :, None] / NY
    coord_z = jnp.arange(NZ, dtype=jnp.float32)[None, None, None, :] / NZ
    rising = 0.5 + 1.5 * (coord_x + coord_y + coord_z) / 3.0
    rough = coarse_rough(key)
    noise = jax.random.truncated_normal(jax.random.fold_in(key, 7), -5.0, 5.0, shape, jnp.float32)
    return (rising * noise + rough).astype(jnp.float32)


def touch_ends(array, key, smallest, largest):
    spot = [jax.random.randint(jax.random.fold_in(key, axis), (), 0, length) for axis, length in enumerate(array.shape)]
    widest = array.shape.index(max(array.shape))
    next_to = spot[:widest] + [(spot[widest] + 1) % array.shape[widest]] + spot[widest + 1:]
    return array.at[tuple(spot)].set(smallest).at[tuple(next_to)].set(largest)


def setup_inputs(seed: int = 0) -> dict:
    seeds = jax.random.split(jax.random.key(seed), 3)
    return {
        "fields": draw_fields(jax.random.fold_in(seeds[2], 71), 0),
        "exponents": touch_ends(jax.random.randint(seeds[1], (LEVELS,), -5, 0), jax.random.fold_in(seeds[1], 1), -5, -1).astype(jnp.int32),
    }


def split_pair(values, axis_dim):
    length = values.shape[axis_dim]
    even_part = lax.slice_in_dim(values, 0, length, 2, axis_dim)
    odd_part = lax.slice_in_dim(values, 1, length, 2, axis_dim)
    return even_part, odd_part


def lift_whole(values, axis_dim):
    even_part, odd_part = split_pair(values, axis_dim)
    detail = odd_part - 0.5 * (even_part + jnp.roll(even_part, -1, axis_dim))
    smooth = even_part + 0.25 * (jnp.roll(detail, 1, axis_dim) + detail)
    return jnp.stack((smooth, detail), axis_dim + 1).reshape(values.shape)


def detail_mask(shape):
    parity_flags = [(jnp.arange(shape[index_dim]) % 2) == 0 for index_dim in (1, 2, 3)]
    smooth_cells = parity_flags[0][:, None, None] & parity_flags[1][None, :, None] & parity_flags[2][None, None, :]
    return jnp.where(smooth_cells, 0.0, 1.0).astype(jnp.float32)[None]


def shrink(values, exponent):
    thresh = jnp.exp2(exponent.astype(jnp.float32))
    return jnp.sign(values) * jnp.maximum(jnp.abs(values) - thresh, 0.0)


def reference(fields, exponents):
    current = fields
    layers = []
    energies = []
    retained = []
    cell_total = NX * NY * NZ
    for layer_index in range(FINE + COARSE):
        for axis_dim in (1, 2, 3):
            current = lift_whole(current, axis_dim)
        masking = detail_mask(current.shape)
        shrunk = shrink(current, exponents[layer_index])
        level_count = 7.0 * cell_total / 8 ** (layer_index + 1)
        energies.append(jnp.sum(current * current * masking, axis=(1, 2, 3)) / level_count)
        retained.append(jnp.sum(jnp.abs(shrunk) * masking, axis=(1, 2, 3)) / level_count)
        layers.append(shrunk)
        current = current[:, ::2, ::2, ::2]
    result = current
    for shrunk in reversed(layers):
        result = shrunk.at[:, ::2, ::2, ::2].set(result)
    statistics = jnp.stack((jnp.stack(energies, 1), jnp.stack(retained, 1)))
    return result, statistics
```

```python
import functools

import numpy as np

import jax
import jax.numpy as jnp
from jax import lax
from jax.experimental import pallas as pl
from jax.experimental.pallas import tpu as pltpu
from jax.sharding import PartitionSpec as P

FINE = 3
LEVELS = 5
LANES = 128
MESH = pl.DeviceIdType.MESH


def periodic_lift(length):
    eye = np.eye(length)
    even, odd = eye[0::2], eye[1::2]
    detail = odd - 0.5 * (even + np.roll(even, -1, 0))
    smooth = even + 0.25 * (np.roll(detail, 1, 0) + detail)
    whole = np.zeros((length, length))
    whole[0::2] = smooth
    whole[1::2] = detail
    return whole


def second_lift(length):
    whole = np.zeros((length, length))
    whole[0::2, 0::2] = periodic_lift(length // 2)
    return whole


def coarse_matrices(sizes, coarse):
    nx, ny, nz = sizes
    cx, cy, cz = coarse
    rows = np.arange(nx * ny * cx * cy)
    dev, inner = rows // (cx * cy), rows % (cx * cy)
    gx = (dev // ny) * cx + inner // cy
    gy = (dev % ny) * cy + inner % cy
    step = LANES // cz
    lanes = np.array([z * step + d for d in range(nz) for z in range(cz)])
    result = []
    for make in (periodic_lift, second_lift):
        mx, my, mz = make(nx * cx), make(ny * cy), make(nz * cz)
        both = mx[gx[:, None], gx[None]] * my[gy[:, None], gy[None]]
        along = np.zeros((LANES, LANES))
        along[np.ix_(lanes, lanes)] = mz.T
        result += [both.astype(np.float32), along.astype(np.float32)]
    return result


def iota(shape, axis):
    return lax.broadcasted_iota(jnp.int32, shape, axis)


def roll(values, shift, axis):
    return pltpu.roll(values, shift % values.shape[axis], axis)


def lift_rows(v, low, high):
    n = v.shape[0]
    row = iota(v.shape, 0)
    odd = row % 2 == 1
    up = jnp.where(row == n - 1, high, roll(v, -1, 0))
    w = jnp.where(odd, v - 0.5 * (roll(v, 1, 0) + up), v)
    down = jnp.where(row == 0, low - 0.5 * v, roll(w, 1, 0))
    return jnp.where(odd, w, w + 0.25 * (down + roll(w, -1, 0)))


def lift_lanes(v, rim, s):
    lane = iota(v.shape, 1)
    up = jnp.where(lane == LANES - s, rim, roll(v, -s, 1))
    w = jnp.where(lane % (2 * s) == s, v - 0.5 * (roll(v, s, 1) + up), v)
    down = jnp.where(lane == 0, rim - 0.5 * v, roll(w, s, 1))
    return jnp.where(lane % (2 * s) == 0, w + 0.25 * (down + roll(w, -s, 1)), w)


def shrink(v, thresh):
    return v - jnp.clip(v, -thresh, thresh)


def kernel(sizes, cells, exps, field, k3, l3, k4, l4, out, stats, *scratch):
    nx, ny, nz = sizes
    ndev = nx * ny * nz
    scratch = list(scratch)
    me = (lax.axis_index("gx"), lax.axis_index("gy"), lax.axis_index("gz"))

    def device(dx, dy, dz):
        return (
            lax.rem(me[0] + (dx + nx), nx),
            lax.rem(me[1] + (dy + ny), ny),
            lax.rem(me[2] + (dz + nz), nz),
        )

    def thresh(level):
        return jnp.exp2(jnp.full((1, LANES), exps[level].astype(jnp.float32)))

    def split(j):
        return j // (ny * nz), (j // nz) % ny, j % nz

    barrier = pltpu.get_barrier_semaphore()

    def greet(j, carry):
        pl.semaphore_signal(barrier, inc=1, device_id=device(*split(j)), device_id_type=MESH)
        return carry

    lax.fori_loop(1, ndev, greet, 0)
    gath, msg, rows_s, final_s, g_send, g_recv = scratch[-6:]
    sums = []

    for level in range(FINE):
        (xs, xr, ys, yr, es, er, yl, zs, zr, work, nxt, xy_send, xy_recv, z_send, z_recv) = scratch[
            level * 15 : level * 15 + 15
        ]
        s = 2**level
        n = field.shape[2] // s
        px = field.shape[1] // s
        src = field.at[0] if level == 0 else scratch[(level - 1) * 15 + 10]

        e_plane = src[0]
        p_plane = src[px - 1] - 0.5 * src[px - 2]
        xs[0] = e_plane
        xs[1] = p_plane
        ys[0] = src[:, 0, :]
        ys[1] = src[:, n - 1, :] - 0.5 * src[:, n - 2, :]
        for a, plane in ((0, e_plane), (1, p_plane)):
            es[2 * a] = plane[0:1]
            es[2 * a + 1] = plane[n - 1 : n] - 0.5 * plane[n - 2 : n - 1]
        if level == 0:
            pl.semaphore_wait(barrier, ndev - 1)
        away = (-1, 1)
        copies = []
        for i, (a, b) in enumerate(((0, 0), (0, 1), (1, 0), (1, 1))):
            copies.append((es.at[2 * a + b], er.at[2 * a + b], (away[a], away[b], 0)))
        for b in (0, 1):
            copies.append((ys.at[b], yr.at[b], (0, away[b], 0)))
        for a in (0, 1):
            copies.append((xs.at[a], xr.at[a], (away[a], 0, 0)))
        flights = [
            pltpu.make_async_remote_copy(
                src_ref=f, dst_ref=t, send_sem=xy_send.at[i], recv_sem=xy_recv.at[i],
                device_id=device(*d), device_id_type=MESH,
            )
            for i, (f, t, d) in enumerate(copies)
        ]
        for flight in flights:
            flight.start()
        for flight in flights:
            flight.wait()

        for b in (0, 1):
            yl[b] = lift_rows(yr[b], er[2 + b], er[b])

        lane = iota((n, LANES), 1)

        def slot(x):
            return (x // s) * (2 * s) + x % s

        def plane_step(x, v, packed):
            v = lift_rows(v, yl[1, pl.ds(x, 1), :], yl[0, pl.ds(x, 1), :])
            work[x] = v
            u = jnp.where(lane == LANES - s, v - 0.5 * roll(v, s, 1), v)
            a = slot(x)
            mine = (lane == a) | (lane == a + s)
            return jnp.where(mine, pltpu.roll(u, lax.rem(a + s, LANES), 1), packed)

        def pair_step(k, even, after, before, packed):
            detail = src[2 * k + 1] - 0.5 * (even + after)
            smooth = even + 0.25 * (before + detail)
            packed = plane_step(2 * k, smooth, packed)
            packed = plane_step(2 * k + 1, detail, packed)
            return detail, packed

        def pair_loop(k, carry):
            even, before, packed = carry
            after = src[2 * k + 2]
            detail, packed = pair_step(k, even, after, before, packed)
            return after, detail, packed

        first = src[0]
        carry = (first, xr[1] - 0.5 * first, jnp.zeros((n, LANES), jnp.float32))
        even, before, packed = lax.fori_loop(0, px // 2 - 1, pair_loop, carry, unroll=3)
        _, packed = pair_step(px // 2 - 1, even, xr[0], before, packed)
        zs[...] = packed
        flights = [
            pltpu.make_async_remote_copy(
                src_ref=zs, dst_ref=zr.at[i], send_sem=z_send.at[i], recv_sem=z_recv.at[i],
                device_id=device(0, 0, away[i]), device_id_type=MESH,
            )
            for i in (0, 1)
        ]
        for flight in flights:
            flight.start()
        for flight in flights:
            flight.wait()
        rim = jnp.where(lane % (2 * s) < s, roll(zr[0], -s, 1), roll(zr[1], s, 1))
        level_thresh = thresh(level)
        inner = (lane % (2 * s) == 0) & (iota((n, LANES), 0) % 2 == 0)
        active = lane % s == 0

        def z_step(x, energy, kept, is_even):
            h = pltpu.roll(rim, LANES - s - slot(x), 1)
            v = lift_lanes(work[x], h, s)
            small = shrink(v, level_thresh)
            use = active & ~inner if is_even else active
            energy += jnp.where(use, v * v, 0.0)
            kept += jnp.where(use, jnp.abs(small), 0.0)
            if level == 0:
                out[0, x] = small
            else:
                spot = (0, s * x, pl.ds(0, n, stride=s), slice(None))
                out[spot] = jnp.where(active, small, out[spot])
            return v, energy, kept

        def z_loop(k, carry):
            energy, kept = carry
            v, energy, kept = z_step(2 * k, energy, kept, True)
            work[2 * k] = v
            nxt[k] = work[2 * k, pl.ds(0, n // 2, stride=2), :]
            _, energy, kept = z_step(2 * k + 1, energy, kept, False)
            return energy, kept

        zero = jnp.zeros((n, LANES), jnp.float32)
        energy, kept = lax.fori_loop(0, px // 2, z_loop, (zero, zero), unroll=2)
        sums += [energy, kept]

    last = scratch[(FINE - 1) * 15 + 10]
    cx, cy = last.shape[0], last.shape[1]
    step = 2**FINE
    count = cx * cy
    for x in range(cx):
        rows_s[pl.ds(x * cy, cy), :] = last[x]
    here = rows_s[...]
    lane = iota((count, LANES), 1)
    row = iota((count, LANES), 0)
    here = jnp.where(lane % step == 0, here, 0.0)
    for bit in (1, 2, 4):
        here = jnp.where((row & bit) != 0, roll(here, bit, 1), here)
    groups = count // 8
    one = iota((1, LANES), 1)
    for g in range(groups):
        msg[g : g + 1] = jnp.sum(here[8 * g : 8 * g + 8], axis=0, keepdims=True)
    tail = jnp.zeros((1, LANES), jnp.float32)
    for i, total in enumerate(sums):
        whole = jnp.sum(jnp.sum(total, axis=0, keepdims=True), axis=1, keepdims=True)
        tail = jnp.where(one == i, whole, tail)
    msg[groups:] = jnp.broadcast_to(tail, (msg.shape[0] - groups, LANES))
    flat = (me[0] * ny + me[1]) * nz + me[2]

    def post(j):
        return pltpu.make_async_remote_copy(
            src_ref=msg, dst_ref=gath.at[flat], send_sem=g_send.at[j], recv_sem=g_recv.at[j],
            device_id=device(*split(j)), device_id_type=MESH,
        )

    def send(j, carry):
        post(ndev - j).start()
        return carry

    def settle(j, carry):
        post(j).wait()
        return carry

    lax.fori_loop(1, ndev, send, 0)
    gath[flat] = msg[...]
    lax.fori_loop(1, ndev, settle, 0)

    sub = iota((8, LANES), 0)
    lane8 = iota((8, LANES), 1)

    def unpack(d, tail):
        for g in range(groups):
            acc = jnp.zeros((8, LANES), jnp.float32)
            for z in range(nz):
                v = jnp.broadcast_to(gath[d * nz + z, g : g + 1, :], (8, LANES))
                for bit in (1, 2, 4):
                    v = jnp.where((sub & bit) != 0, roll(v, -bit, 1), v)
                acc += roll(jnp.where(lane8 % step == 0, v, 0.0), z, 1)
            final_s[pl.ds(pl.multiple_of(d * count + 8 * g, 8), 8), :] = acc
        for z in range(nz):
            tail += gath[d * nz + z, groups : groups + 1, :]
        return tail

    tail = lax.fori_loop(0, nx * ny, unpack, jnp.zeros((1, LANES), jnp.float32))

    def dot(a, b):
        return jnp.dot(a, b, precision=lax.Precision.HIGHEST, preferred_element_type=jnp.float32)

    grid = final_s[...]
    grid = dot(dot(k3[...], grid), l3[...])
    grid4 = dot(dot(k4[...], grid), l4[...])
    row = iota(grid.shape, 0)
    lane = iota(grid.shape, 1)
    inner_row = row % count
    gx, gy, gz = inner_row // cy, inner_row % cy, lane // step
    valid = lane % step < nz
    even3 = (gx % 2 == 0) & (gy % 2 == 0) & (gz % 2 == 0)
    even4 = (gx % 4 == 0) & (gy % 4 == 0) & (gz % 4 == 0)
    det3 = valid & ~even3
    det4 = valid & even3 & ~even4
    small3 = shrink(grid, thresh(FINE))
    small4 = shrink(grid4, thresh(FINE + 1))
    final_s[...] = jnp.where(even3, jnp.where(even4, grid4, small4), small3)

    def total(mask, v):
        return jnp.sum(jnp.sum(jnp.where(mask, v, 0.0), axis=0, keepdims=True), axis=1, keepdims=True)

    coarse = ((total(det3, grid * grid), total(det3, jnp.abs(small3))),
              (total(det4, grid4 * grid4), total(det4, jnp.abs(small4))))
    for q in (0, 1):
        line = jnp.zeros((1, LANES), jnp.float32)
        for level in range(LEVELS):
            weight = 8.0 ** (level + 1) / (7.0 * cells)
            if level < FINE:
                value = jnp.sum(jnp.where(one == 2 * level + q, tail, 0.0), axis=1, keepdims=True)
            else:
                value = coarse[level - FINE][q]
            line = jnp.where(one == level, value * weight, line)
        stats[q] = line[:, 0:LEVELS]

    first = pl.multiple_of((me[0] * ny + me[1]) * count, count)
    mine = pltpu.roll(final_s[pl.ds(first, count), :], lax.rem(LANES - me[2], LANES), 1)
    rows_s[...] = mine
    keep = iota((cy, LANES), 1) % step == 0
    for x in range(cx):
        spot = (0, step * x, pl.ds(0, cy, stride=step), slice(None))
        out[spot] = jnp.where(keep, rows_s[pl.ds(x * cy, cy), :], out[spot])


def shards(sizes, fields, exponents):
    nx, ny, nz = sizes
    ndev = nx * ny * nz
    _, lx, ly, lz = fields.shape
    cells = fields.size * ndev
    step = 2**FINE
    coarse = (lx // step, ly // step, lz // step)
    count = coarse[0] * coarse[1]
    tables = coarse_matrices(sizes, coarse)
    scratch = []
    for level in range(FINE):
        x, y = lx >> level, ly >> level
        scratch += [
            pltpu.VMEM((2, y, LANES), jnp.float32),
            pltpu.VMEM((2, y, LANES), jnp.float32),
            pltpu.VMEM((2, x, LANES), jnp.float32),
            pltpu.VMEM((2, x, LANES), jnp.float32),
            pltpu.VMEM((4, 1, LANES), jnp.float32),
            pltpu.VMEM((4, 1, LANES), jnp.float32),
            pltpu.VMEM((2, x, LANES), jnp.float32),
            pltpu.VMEM((y, LANES), jnp.float32),
            pltpu.VMEM((2, y, LANES), jnp.float32),
            pltpu.VMEM((x, y, LANES), jnp.float32),
            pltpu.VMEM((x // 2, y // 2, LANES), jnp.float32),
            pltpu.SemaphoreType.DMA((8,)),
            pltpu.SemaphoreType.DMA((8,)),
            pltpu.SemaphoreType.DMA((2,)),
            pltpu.SemaphoreType.DMA((2,)),
        ]
    height = -(-(count // 8 + 1) // 4) * 4
    scratch += [
        pltpu.VMEM((ndev, height, LANES), jnp.float32),
        pltpu.VMEM((height, LANES), jnp.float32),
        pltpu.VMEM((count, LANES), jnp.float32),
        pltpu.VMEM((nx * ny * count, LANES), jnp.float32),
        pltpu.SemaphoreType.DMA((ndev,)),
        pltpu.SemaphoreType.DMA((ndev,)),
    ]
    vmem = pl.BlockSpec(memory_space=pltpu.VMEM)
    return pl.pallas_call(
        functools.partial(kernel, sizes, cells),
        out_shape=(
            jax.ShapeDtypeStruct(fields.shape, jnp.float32),
            jax.ShapeDtypeStruct((2, 1, LEVELS), jnp.float32),
        ),
        in_specs=[pl.BlockSpec(memory_space=pltpu.SMEM)] + [vmem] * 5,
        out_specs=(vmem, vmem),
        scratch_shapes=scratch,
        compiler_params=pltpu.CompilerParams(
            collective_id=0, has_side_effects=True, vmem_limit_bytes=48 * 2**20
        ),
    )(exponents, fields, *tables)


def solution(mesh):
    sizes = tuple(mesh.shape[name] for name in ("gx", "gy", "gz"))
    placed = (P(None, "gx", "gy", "gz"), P())
    return jax.shard_map(
        functools.partial(shards, sizes),
        mesh=mesh,
        in_specs=placed,
        out_specs=placed,
        check_vma=False,
    )
```

```python
import functools

import numpy as np

import jax
import jax.numpy as jnp
from jax import lax
from jax.experimental import pallas as pl
from jax.experimental.pallas import tpu as pltpu
from jax.sharding import PartitionSpec as P

FINE = 3
LEVELS = 5
LANES = 128
BUFFERS = 19
VMEM_LIMIT = 67_043_328
MESH = pl.DeviceIdType.MESH


def periodic_lift(length):
    eye = np.eye(length)
    even, odd = eye[0::2], eye[1::2]
    detail = odd - 0.5 * (even + np.roll(even, -1, 0))
    smooth = even + 0.25 * (np.roll(detail, 1, 0) + detail)
    whole = np.zeros((length, length))
    whole[0::2] = smooth
    whole[1::2] = detail
    return whole


def second_lift(length):
    whole = np.zeros((length, length))
    whole[0::2, 0::2] = periodic_lift(length // 2)
    return whole


def coarse_matrices(sizes, coarse):
    nx, ny, nz = sizes
    cx, cy, cz = coarse
    rows = np.arange(nx * ny * cx * cy)
    dev, inner = rows // (cx * cy), rows % (cx * cy)
    gx = (dev // ny) * cx + inner // cy
    gy = (dev % ny) * cy + inner % cy
    step = LANES // cz
    lanes = np.array([z * step + d for d in range(nz) for z in range(cz)])
    result = []
    for make in (periodic_lift, second_lift):
        mx, my, mz = make(nx * cx), make(ny * cy), make(nz * cz)
        both = mx[gx[:, None], gx[None]] * my[gy[:, None], gy[None]]
        along = np.zeros((LANES, LANES))
        along[np.ix_(lanes, lanes)] = mz.T
        result.append((both.astype(np.float32), along.astype(np.float32)))
    return [np.stack(pair) for pair in zip(*result)]


def iota(shape, axis):
    return lax.broadcasted_iota(jnp.int32, shape, axis)


def roll(values, shift, axis):
    return pltpu.roll(values, shift % values.shape[axis], axis)


def lift_rows(v, low, high):
    n = v.shape[0]
    row = iota(v.shape, 0)
    odd = row % 2 == 1
    up = jnp.where(row == n - 1, high, roll(v, -1, 0))
    w = jnp.where(odd, v - 0.5 * (roll(v, 1, 0) + up), v)
    down = jnp.where(row == 0, low - 0.5 * v, roll(w, 1, 0))
    return jnp.where(odd, w, w + 0.25 * (down + roll(w, -1, 0)))


def lift_lanes(v, rim, s):
    lane = iota(v.shape, 1)
    up = jnp.where(lane == LANES - s, rim, roll(v, -s, 1))
    w = jnp.where(lane % (2 * s) == s, v - 0.5 * (roll(v, s, 1) + up), v)
    down = jnp.where(lane == 0, rim - 0.5 * v, roll(w, s, 1))
    return jnp.where(lane % (2 * s) == 0, w + 0.25 * (down + roll(w, -s, 1)), w)


def shrink(v, thresh):
    return v - jnp.clip(v, -thresh, thresh)


def kernel(sizes, cells, exps_in, field_in, rows_in, lanes_in, out, stats, *scratch):
    nx, ny, nz = sizes
    ndev = nx * ny * nz
    scratch = list(scratch)
    field, exps, k_s, l_s, in_sem = scratch[-5:]
    scratch = scratch[:-5]
    loads = [
        pltpu.make_async_copy(a, b, in_sem.at[i])
        for i, (a, b) in enumerate(((field_in, field), (exps_in, exps), (rows_in, k_s), (lanes_in, l_s)))
    ]
    for load in loads:
        load.start()
    me = (lax.axis_index("gx"), lax.axis_index("gy"), lax.axis_index("gz"))

    def device(dx, dy, dz):
        return (
            lax.rem(me[0] + (dx + nx), nx),
            lax.rem(me[1] + (dy + ny), ny),
            lax.rem(me[2] + (dz + nz), nz),
        )

    def thresh(level):
        return jnp.exp2(jnp.full((1, LANES), exps[level].astype(jnp.float32)))

    def split(j):
        return j // (ny * nz), (j // nz) % ny, j % nz

    barrier = pltpu.get_barrier_semaphore()

    near = max(sizes) // 2 <= FINE
    greeted = {
        tuple((d + size - 1) % size if near else d for d, size in zip(spot, sizes))
        for spot in np.ndindex(*(3, 3, 3) if near else sizes)
    } - {(0, 0, 0)}
    for spot in sorted(greeted):
        pl.semaphore_signal(barrier, inc=1, device_id=device(*spot), device_id_type=MESH)
    gath, msg, rows_s, final_s, g_send, g_recv = scratch[-6:]
    sums = []
    loads[0].wait()
    loads[1].wait()
    away = (-1, 1)
    alone = nx == 2

    for level in range(FINE):
        (xs, xr, ys, yr, es, er, yl, zs, zr, hs, hr, ds, dr, cs, cr, work, nxt, send_sem, recv_sem) = scratch[
            level * BUFFERS : level * BUFFERS + BUFFERS
        ]
        s = 2**level
        n = field.shape[2] // s
        px = field.shape[1] // s
        src = field.at[0] if level == 0 else scratch[(level - 1) * BUFFERS + 16]
        lane = iota((n, LANES), 1)

        def edge(v):
            return v[0:1], v[n - 1 : n] - 0.5 * v[n - 2 : n - 1]

        e_plane = src[0]
        p_plane = src[px - 1] - 0.5 * src[px - 2]
        xs[0] = e_plane
        xs[1] = p_plane
        ys[0] = src[:, 0, :]
        ys[1] = src[:, n - 1, :] - 0.5 * src[:, n - 2, :]
        for a, plane in ((0, e_plane), (1, p_plane)):
            es[2 * a], es[2 * a + 1] = edge(plane)

        packed = jnp.zeros((n, LANES), jnp.float32)
        for x in range(px):
            v = src[x]
            u = jnp.where(lane == LANES - s, v - 0.5 * roll(v, s, 1), v)
            at = 2 * s * x
            packed = jnp.where((lane == at) | (lane == at + s), roll(u, at + s, 1), packed)
        half = 2 * s * px
        combined = packed - 0.5 * roll(packed, 2 * s, 1)
        sides = roll(jnp.where(lane < half // 2, packed, combined), half, 1)
        zs[...] = packed
        hs[...] = sides
        ds[0], ds[1] = edge(packed)
        cs[0], cs[1] = edge(sides)

        if level == 0:
            pl.semaphore_wait(barrier, len(greeted))
        copies = []
        ways = (0,) if alone else (0, 1)
        for i in (0, 1):
            for b in (0, 1):
                for a in ways:
                    copies.append((cs.at[b], cr.at[4 * a + 2 * b + i], (away[a], away[b], away[i])))
                copies.append((ds.at[b], dr.at[2 * b + i], (0, away[b], away[i])))
        for a in (0, 1):
            for b in (0, 1):
                copies.append((es.at[2 * a + b], er.at[2 * a + b], (away[a], away[b], 0)))
        for b in (0, 1):
            copies.append((ys.at[b], yr.at[b], (0, away[b], 0)))
        for i in (0, 1):
            for a in ways:
                copies.append((hs, hr.at[2 * a + i], (away[a], 0, away[i])))
        for a in (0, 1):
            copies.append((xs.at[a], xr.at[a], (away[a], 0, 0)))
        for i in (0, 1):
            copies.append((zs, zr.at[i], (0, 0, away[i])))
        flights = [
            pltpu.make_async_remote_copy(
                src_ref=f, dst_ref=t, send_sem=send_sem.at[i], recv_sem=recv_sem.at[i],
                device_id=device(*d), device_id_type=MESH,
            )
            for i, (f, t, d) in enumerate(copies)
        ]
        for flight in flights:
            flight.start()
        for flight in flights:
            flight.wait()

        for b in (0, 1):
            yl[b] = lift_rows(yr[b], er[2 + b], er[b])

        def rim_of(main, side):
            spot = iota(main(0).shape, 1)
            parts = []
            for i in (0, 1):
                after = side(0, i)
                before = after if alone else side(1, i)
                v = jnp.where(spot < half, main(i), 0.0)
                v = jnp.where((spot >= half) & (spot < half + 2 * s), after, v)
                parts.append(jnp.where(spot >= LANES - 2 * s, before, v))
            v = jnp.where(spot % (2 * s) < s, roll(parts[0], -s, 1), roll(parts[1], s, 1))
            odd = (spot // (2 * s)) % 2 == 1
            w = jnp.where(odd, v - 0.5 * (roll(v, 2 * s, 1) + roll(v, -2 * s, 1)), v)
            return jnp.where(odd, w, w + 0.25 * (roll(w, 2 * s, 1) + roll(w, -2 * s, 1)))

        rim_rows = [
            rim_of(lambda i: dr[2 * b + i], lambda a, i: cr[4 * a + 2 * b + i]) for b in (0, 1)
        ]
        rim = rim_of(lambda i: zr[i], lambda a, i: hr[2 * a + i])
        rim = lift_rows(rim, rim_rows[1], rim_rows[0])
        level_thresh = thresh(level)
        inner = (lane % (2 * s) == 0) & (iota((n, LANES), 0) % 2 == 0)
        active = lane % s == 0

        energy = kept = jnp.zeros((n, LANES), jnp.float32)

        def plane_step(x, v, energy, kept):
            v = lift_rows(v, yl[1, x : x + 1, :], yl[0, x : x + 1, :])
            v = lift_lanes(v, roll(rim, LANES - s - 2 * s * x, 1), s)
            small = shrink(v, level_thresh)
            use = active & ~inner if x % 2 == 0 else active
            energy += jnp.where(use, v * v, 0.0)
            kept += jnp.where(use, jnp.abs(small), 0.0)
            if level == 0:
                out[0, x] = small
            else:
                spot = (0, s * x, pl.ds(0, n, stride=s), slice(None))
                out[spot] = jnp.where(active, small, out[spot])
            if x % 2 == 0:
                work[x // 2] = v
                nxt[x // 2] = work[x // 2, pl.ds(0, n // 2, stride=2), :]
            return energy, kept

        even = src[0]
        before = xr[1] - 0.5 * even
        for k in range(px // 2):
            after = src[2 * k + 2] if 2 * k + 2 < px else xr[0]
            detail = src[2 * k + 1] - 0.5 * (even + after)
            smooth = even + 0.25 * (before + detail)
            energy, kept = plane_step(2 * k, smooth, energy, kept)
            energy, kept = plane_step(2 * k + 1, detail, energy, kept)
            even, before = after, detail
        sums += [energy, kept]

    last = scratch[(FINE - 1) * BUFFERS + 16]
    cx, cy = last.shape[0], last.shape[1]
    step = 2**FINE
    count = cx * cy
    for x in range(cx):
        rows_s[pl.ds(x * cy, cy), :] = last[x]
    here = rows_s[...]
    lane = iota((count, LANES), 1)
    row = iota((count, LANES), 0)
    here = jnp.where(lane % step == 0, here, 0.0)
    for bit in (1, 2, 4):
        here = jnp.where((row & bit) != 0, roll(here, bit, 1), here)
    groups = count // 8
    one = iota((1, LANES), 1)
    for g in range(groups):
        msg[g : g + 1] = jnp.sum(here[8 * g : 8 * g + 8], axis=0, keepdims=True)
    tail = jnp.zeros((1, LANES), jnp.float32)
    for i, total in enumerate(sums):
        whole = jnp.sum(jnp.sum(total, axis=0, keepdims=True), axis=1, keepdims=True)
        tail = jnp.where(one == i, whole, tail)
    msg[groups:] = jnp.broadcast_to(tail, (msg.shape[0] - groups, LANES))
    flat = (me[0] * ny + me[1]) * nz + me[2]

    def post(j):
        return pltpu.make_async_remote_copy(
            src_ref=msg, dst_ref=gath.at[flat], send_sem=g_send.at[j], recv_sem=g_recv.at[j],
            device_id=device(*split(j)), device_id_type=MESH,
        )

    def send(j, carry):
        post(ndev - j).start()
        return carry

    def settle(j, carry):
        post(j).wait()
        return carry

    lax.fori_loop(1, ndev, send, 0)
    gath[flat] = msg[...]
    lax.fori_loop(1, ndev, settle, 0)

    sub = iota((8, LANES), 0)
    lane8 = iota((8, LANES), 1)

    def unpack(d, tail):
        for g in range(groups):
            acc = jnp.zeros((8, LANES), jnp.float32)
            for z in range(nz):
                v = jnp.broadcast_to(gath[d * nz + z, g : g + 1, :], (8, LANES))
                for bit in (1, 2, 4):
                    v = jnp.where((sub & bit) != 0, roll(v, -bit, 1), v)
                acc += roll(jnp.where(lane8 % step == 0, v, 0.0), z, 1)
            final_s[pl.ds(pl.multiple_of(d * count + 8 * g, 8), 8), :] = acc
        for z in range(nz):
            tail += gath[d * nz + z, groups : groups + 1, :]
        return tail

    tail = lax.fori_loop(0, nx * ny, unpack, jnp.zeros((1, LANES), jnp.float32))

    def dot(a, b):
        return jnp.dot(a, b, precision=lax.Precision.HIGHEST, preferred_element_type=jnp.float32)

    grid = final_s[...]
    loads[2].wait()
    loads[3].wait()
    grid = dot(dot(k_s[0], grid), l_s[0])
    grid4 = dot(dot(k_s[1], grid), l_s[1])
    row = iota(grid.shape, 0)
    lane = iota(grid.shape, 1)
    inner_row = row % count
    gx, gy, gz = inner_row // cy, inner_row % cy, lane // step
    valid = lane % step < nz
    even3 = (gx % 2 == 0) & (gy % 2 == 0) & (gz % 2 == 0)
    even4 = (gx % 4 == 0) & (gy % 4 == 0) & (gz % 4 == 0)
    det3 = valid & ~even3
    det4 = valid & even3 & ~even4
    small3 = shrink(grid, thresh(FINE))
    small4 = shrink(grid4, thresh(FINE + 1))
    final_s[...] = jnp.where(even3, jnp.where(even4, grid4, small4), small3)

    def total(mask, v):
        return jnp.sum(jnp.sum(jnp.where(mask, v, 0.0), axis=0, keepdims=True), axis=1, keepdims=True)

    coarse = ((total(det3, grid * grid), total(det3, jnp.abs(small3))),
              (total(det4, grid4 * grid4), total(det4, jnp.abs(small4))))
    for q in (0, 1):
        line = jnp.zeros((1, LANES), jnp.float32)
        for level in range(LEVELS):
            weight = 8.0 ** (level + 1) / (7.0 * cells)
            if level < FINE:
                value = jnp.sum(jnp.where(one == 2 * level + q, tail, 0.0), axis=1, keepdims=True)
            else:
                value = coarse[level - FINE][q]
            line = jnp.where(one == level, value * weight, line)
        stats[q] = line[:, 0:LEVELS]

    first = pl.multiple_of((me[0] * ny + me[1]) * count, count)
    mine = pltpu.roll(final_s[pl.ds(first, count), :], lax.rem(LANES - me[2], LANES), 1)
    rows_s[...] = mine
    keep = iota((cy, LANES), 1) % step == 0
    for x in range(cx):
        spot = (0, step * x, pl.ds(0, cy, stride=step), slice(None))
        out[spot] = jnp.where(keep, rows_s[pl.ds(x * cy, cy), :], out[spot])


def shards(sizes, fields, exponents):
    nx, ny, nz = sizes
    ndev = nx * ny * nz
    _, lx, ly, lz = fields.shape
    cells = fields.size * ndev
    step = 2**FINE
    coarse = (lx // step, ly // step, lz // step)
    count = coarse[0] * coarse[1]
    tables = coarse_matrices(sizes, coarse)
    scratch = []
    for level in range(FINE):
        x, y = lx >> level, ly >> level
        scratch += [
            *(pltpu.VMEM(shape, jnp.float32) for shape in (
                (2, y, LANES), (2, y, LANES), (2, x, LANES), (2, x, LANES), (4, 1, LANES), (4, 1, LANES),
                (2, x, LANES), (y, LANES), (2, y, LANES), (y, LANES), (4, y, LANES), (2, 1, LANES),
                (4, 1, LANES), (2, 1, LANES), (8, 1, LANES), (x // 2, y, LANES), (x // 2, y // 2, LANES),
            )),
            pltpu.SemaphoreType.DMA((26,)),
            pltpu.SemaphoreType.DMA((26,)),
        ]
    height = -(-(count // 8 + 1) // 4) * 4
    scratch += [
        pltpu.VMEM((ndev, height, LANES), jnp.float32),
        pltpu.VMEM((height, LANES), jnp.float32),
        pltpu.VMEM((count, LANES), jnp.float32),
        pltpu.VMEM((nx * ny * count, LANES), jnp.float32),
        pltpu.SemaphoreType.DMA((ndev,)),
        pltpu.SemaphoreType.DMA((ndev,)),
        pltpu.VMEM(fields.shape, jnp.float32),
        pltpu.SMEM(exponents.shape, jnp.int32),
        pltpu.VMEM(tables[0].shape, jnp.float32),
        pltpu.VMEM(tables[1].shape, jnp.float32),
        pltpu.SemaphoreType.DMA((4,)),
    ]
    vmem = pl.BlockSpec(memory_space=pltpu.VMEM)
    return pl.pallas_call(
        functools.partial(kernel, sizes, cells),
        out_shape=(
            jax.ShapeDtypeStruct(fields.shape, jnp.float32),
            jax.ShapeDtypeStruct((2, 1, LEVELS), jnp.float32),
        ),
        in_specs=[pl.BlockSpec(memory_space=pltpu.HBM)] * 4,
        out_specs=(vmem, vmem),
        scratch_shapes=scratch,
        compiler_params=pltpu.CompilerParams(
            collective_id=0, has_side_effects=True, vmem_limit_bytes=VMEM_LIMIT
        ),
    )(exponents, fields, *tables)


def solution(mesh):
    sizes = tuple(mesh.shape[name] for name in ("gx", "gy", "gz"))
    placed = (P(None, "gx", "gy", "gz"), P())
    return jax.shard_map(
        functools.partial(shards, sizes),
        mesh=mesh,
        in_specs=placed,
        out_specs=placed,
        check_vma=False,
    )
```

```python
import functools

import numpy as np

import jax
import jax.numpy as jnp
from jax import lax
from jax.experimental import pallas as pl
from jax.experimental.pallas import tpu as pltpu
from jax.sharding import PartitionSpec as P

FINE = 3
LEVELS = 5
LANES = 128
BUFFERS = 19
VMEM_LIMIT = 67_043_328
MESH = pl.DeviceIdType.MESH


def periodic_lift(length):
    eye = np.eye(length)
    even, odd = eye[0::2], eye[1::2]
    detail = odd - 0.5 * (even + np.roll(even, -1, 0))
    smooth = even + 0.25 * (np.roll(detail, 1, 0) + detail)
    whole = np.zeros((length, length))
    whole[0::2] = smooth
    whole[1::2] = detail
    return whole


def second_lift(length):
    whole = np.zeros((length, length))
    whole[0::2, 0::2] = periodic_lift(length // 2)
    return whole


def coarse_matrices(sizes, coarse):
    nx, ny, nz = sizes
    cx, cy, cz = coarse
    rows = np.arange(nx * ny * cx * cy)
    dev, inner = rows // (cx * cy), rows % (cx * cy)
    gx = (dev // ny) * cx + inner // cy
    gy = (dev % ny) * cy + inner % cy
    step = LANES // cz
    lanes = np.array([z * step + d for d in range(nz) for z in range(cz)])
    result = []
    for both_levels in (False, True):
        mx, my, mz = periodic_lift(nx * cx), periodic_lift(ny * cy), periodic_lift(nz * cz)
        if both_levels:
            mx, my, mz = second_lift(nx * cx) @ mx, second_lift(ny * cy) @ my, second_lift(nz * cz) @ mz
        both = mx[gx[:, None], gx[None]] * my[gy[:, None], gy[None]]
        along = np.zeros((LANES, LANES))
        along[np.ix_(lanes, lanes)] = mz.T
        result.append((both.astype(np.float32), along.astype(np.float32)))
    return [np.stack(pair) for pair in zip(*result)]


def iota(shape, axis):
    return lax.broadcasted_iota(jnp.int32, shape, axis)


def roll(values, shift, axis):
    return pltpu.roll(values, shift % values.shape[axis], axis)


def lift_rows(v, low, high):
    n = v.shape[0]
    row = iota(v.shape, 0)
    odd = row % 2 == 1
    up = jnp.where(row == n - 1, high, roll(v, -1, 0))
    w = jnp.where(odd, v - 0.5 * (roll(v, 1, 0) + up), v)
    down = jnp.where(row == 0, low - 0.5 * v, roll(w, 1, 0))
    return jnp.where(odd, w, w + 0.25 * (down + roll(w, -1, 0)))


def lift_lanes(v, rim, s):
    lane = iota(v.shape, 1)
    up = jnp.where(lane == LANES - s, rim, roll(v, -s, 1))
    w = jnp.where(lane % (2 * s) == s, v - 0.5 * (roll(v, s, 1) + up), v)
    down = jnp.where(lane == 0, rim - 0.5 * v, roll(w, s, 1))
    return jnp.where(lane % (2 * s) == 0, w + 0.25 * (down + roll(w, -s, 1)), w)


def shrink(v, thresh):
    return v - jnp.clip(v, -thresh, thresh)


def kernel(sizes, cells, exps_in, field_in, rows_in, lanes_in, out, stats, *scratch):
    nx, ny, nz = sizes
    ndev = nx * ny * nz
    scratch = list(scratch)
    field, exps, k_s, l_s, in_sem = scratch[-5:]
    scratch = scratch[:-5]
    loads = [
        pltpu.make_async_copy(a, b, in_sem.at[i])
        for i, (a, b) in enumerate(((field_in, field), (exps_in, exps), (rows_in, k_s), (lanes_in, l_s)))
    ]
    for load in loads:
        load.start()
    me = (lax.axis_index("gx"), lax.axis_index("gy"), lax.axis_index("gz"))

    def device(dx, dy, dz):
        return (
            lax.rem(me[0] + (dx + nx), nx),
            lax.rem(me[1] + (dy + ny), ny),
            lax.rem(me[2] + (dz + nz), nz),
        )

    def thresh(level):
        return jnp.exp2(jnp.full((1, LANES), exps[level].astype(jnp.float32)))

    def split(j):
        return j // (ny * nz), (j // nz) % ny, j % nz

    barrier = pltpu.get_barrier_semaphore()

    near = max(sizes) // 2 <= FINE
    greeted = {
        tuple((d + size - 1) % size if near else d for d, size in zip(spot, sizes))
        for spot in np.ndindex(*(3, 3, 3) if near else sizes)
    } - {(0, 0, 0)}
    for spot in sorted(greeted):
        pl.semaphore_signal(barrier, inc=1, device_id=device(*spot), device_id_type=MESH)
    gath, msg, rows_s, final_s, g_send, g_recv = scratch[-6:]
    sums = []
    loads[0].wait()
    loads[1].wait()
    away = (-1, 1)
    alone = nx == 2

    for level in range(FINE):
        (xs, xr, ys, yr, es, er, yl, zs, zr, hs, hr, ds, dr, cs, cr, work, nxt, send_sem, recv_sem) = scratch[
            level * BUFFERS : level * BUFFERS + BUFFERS
        ]
        s = 2**level
        n = field.shape[2] // s
        px = field.shape[1] // s
        src = field.at[0] if level == 0 else scratch[(level - 1) * BUFFERS + 16]
        lane = iota((n, LANES), 1)

        def edge(v):
            return v[0:1], v[n - 1 : n] - 0.5 * v[n - 2 : n - 1]

        e_plane = src[0]
        p_plane = src[px - 1] - 0.5 * src[px - 2]
        xs[0] = e_plane
        xs[1] = p_plane
        ys[0] = src[:, 0, :]
        ys[1] = src[:, n - 1, :] - 0.5 * src[:, n - 2, :]
        for a, plane in ((0, e_plane), (1, p_plane)):
            es[2 * a], es[2 * a + 1] = edge(plane)

        packed = jnp.zeros((n, LANES), jnp.float32)
        for x in range(px):
            v = src[x]
            u = jnp.where(lane == LANES - s, v - 0.5 * roll(v, s, 1), v)
            at = 2 * s * x
            packed = jnp.where((lane == at) | (lane == at + s), roll(u, at + s, 1), packed)
        half = 2 * s * px
        combined = packed - 0.5 * roll(packed, 2 * s, 1)
        sides = roll(jnp.where(lane < half // 2, packed, combined), half, 1)
        zs[...] = packed
        hs[...] = sides
        ds[0], ds[1] = edge(packed)
        cs[0], cs[1] = edge(sides)

        if level == 0:
            pl.semaphore_wait(barrier, len(greeted))
        copies = []
        ways = (0,) if alone else (0, 1)
        for i in (0, 1):
            for b in (0, 1):
                for a in ways:
                    copies.append((cs.at[b], cr.at[4 * a + 2 * b + i], (away[a], away[b], away[i])))
                copies.append((ds.at[b], dr.at[2 * b + i], (0, away[b], away[i])))
        for a in (0, 1):
            for b in (0, 1):
                copies.append((es.at[2 * a + b], er.at[2 * a + b], (away[a], away[b], 0)))
        for b in (0, 1):
            copies.append((ys.at[b], yr.at[b], (0, away[b], 0)))
        for i in (0, 1):
            for a in ways:
                copies.append((hs, hr.at[2 * a + i], (away[a], 0, away[i])))
        for a in (0, 1):
            copies.append((xs.at[a], xr.at[a], (away[a], 0, 0)))
        for i in (0, 1):
            copies.append((zs, zr.at[i], (0, 0, away[i])))
        flights = [
            pltpu.make_async_remote_copy(
                src_ref=f, dst_ref=t, send_sem=send_sem.at[i], recv_sem=recv_sem.at[i],
                device_id=device(*d), device_id_type=MESH,
            )
            for i, (f, t, d) in enumerate(copies)
        ]
        for flight in flights:
            flight.start()
        for flight in flights:
            flight.wait()

        for b in (0, 1):
            yl[b] = lift_rows(yr[b], er[2 + b], er[b])

        def rim_of(main, side):
            spot = iota(main(0).shape, 1)
            parts = []
            for i in (0, 1):
                after = side(0, i)
                before = after if alone else side(1, i)
                v = jnp.where(spot < half, main(i), 0.0)
                v = jnp.where((spot >= half) & (spot < half + 2 * s), after, v)
                parts.append(jnp.where(spot >= LANES - 2 * s, before, v))
            v = jnp.where(spot % (2 * s) < s, roll(parts[0], -s, 1), roll(parts[1], s, 1))
            odd = (spot // (2 * s)) % 2 == 1
            w = jnp.where(odd, v - 0.5 * (roll(v, 2 * s, 1) + roll(v, -2 * s, 1)), v)
            return jnp.where(odd, w, w + 0.25 * (roll(w, 2 * s, 1) + roll(w, -2 * s, 1)))

        rim_rows = [
            rim_of(lambda i: dr[2 * b + i], lambda a, i: cr[4 * a + 2 * b + i]) for b in (0, 1)
        ]
        rim = rim_of(lambda i: zr[i], lambda a, i: hr[2 * a + i])
        rim = lift_rows(rim, rim_rows[1], rim_rows[0])
        level_thresh = thresh(level)
        inner = (lane % (2 * s) == 0) & (iota((n, LANES), 0) % 2 == 0)
        active = lane % s == 0

        energy = kept = jnp.zeros((n, LANES), jnp.float32)

        def plane_step(x, v, energy, kept):
            v = lift_rows(v, yl[1, x : x + 1, :], yl[0, x : x + 1, :])
            v = lift_lanes(v, roll(rim, LANES - s - 2 * s * x, 1), s)
            small = shrink(v, level_thresh)
            use = active & ~inner if x % 2 == 0 else active
            energy += jnp.where(use, v * v, 0.0)
            kept += jnp.where(use, jnp.abs(small), 0.0)
            if level == 0:
                out[0, x] = small
            else:
                spot = (0, s * x, pl.ds(0, n, stride=s), slice(None))
                out[spot] = jnp.where(active, small, out[spot])
            if x % 2 == 0:
                work[x // 2] = v
                nxt[x // 2] = work[x // 2, pl.ds(0, n // 2, stride=2), :]
            return energy, kept

        even = src[0]
        before = xr[1] - 0.5 * even
        for k in range(px // 2):
            after = src[2 * k + 2] if 2 * k + 2 < px else xr[0]
            detail = src[2 * k + 1] - 0.5 * (even + after)
            smooth = even + 0.25 * (before + detail)
            energy, kept = plane_step(2 * k, smooth, energy, kept)
            energy, kept = plane_step(2 * k + 1, detail, energy, kept)
            even, before = after, detail
        sums += [energy, kept]

    last = scratch[(FINE - 1) * BUFFERS + 16]
    cx, cy = last.shape[0], last.shape[1]
    step = 2**FINE
    count = cx * cy
    for x in range(cx):
        rows_s[pl.ds(x * cy, cy), :] = last[x]
    here = rows_s[...]
    lane = iota((count, LANES), 1)
    row = iota((count, LANES), 0)
    here = jnp.where(lane % step == 0, here, 0.0)
    for bit in (1, 2, 4):
        here = jnp.where((row & bit) != 0, roll(here, bit, 1), here)
    groups = count // 8
    one = iota((1, LANES), 1)
    for g in range(groups):
        msg[g : g + 1] = jnp.sum(here[8 * g : 8 * g + 8], axis=0, keepdims=True)
    tail = jnp.zeros((1, LANES), jnp.float32)
    for i, total in enumerate(sums):
        whole = jnp.sum(jnp.sum(total, axis=0, keepdims=True), axis=1, keepdims=True)
        tail = jnp.where(one == i, whole, tail)
    msg[groups:] = jnp.broadcast_to(tail, (msg.shape[0] - groups, LANES))
    flat = (me[0] * ny + me[1]) * nz + me[2]

    def post(j):
        return pltpu.make_async_remote_copy(
            src_ref=msg, dst_ref=gath.at[flat], send_sem=g_send.at[j], recv_sem=g_recv.at[j],
            device_id=device(*split(j)), device_id_type=MESH,
        )

    def send(j, carry):
        post(ndev - j).start()
        return carry

    def settle(j, carry):
        post(j).wait()
        return carry

    if ndev <= 32:
        posts = [post(ndev - j) for j in range(1, ndev)]
        for flight in posts:
            flight.start()
        gath[flat] = msg[...]
        for flight in posts:
            flight.wait()
    else:
        lax.fori_loop(1, ndev, send, 0)
        gath[flat] = msg[...]
        lax.fori_loop(1, ndev, settle, 0)

    sub = iota((8, LANES), 0)
    lane8 = iota((8, LANES), 1)

    def unpack(d, tail):
        for g in range(groups):
            acc = jnp.zeros((8, LANES), jnp.float32)
            for z in range(nz):
                v = jnp.broadcast_to(gath[d * nz + z, g : g + 1, :], (8, LANES))
                for bit in (1, 2, 4):
                    v = jnp.where((sub & bit) != 0, roll(v, -bit, 1), v)
                acc += roll(jnp.where(lane8 % step == 0, v, 0.0), z, 1)
            final_s[pl.ds(pl.multiple_of(d * count + 8 * g, 8), 8), :] = acc
        for z in range(nz):
            tail += gath[d * nz + z, groups : groups + 1, :]
        return tail

    tail = lax.fori_loop(0, nx * ny, unpack, jnp.zeros((1, LANES), jnp.float32), unroll=nx * ny <= 8)

    def dot(a, b):
        return jnp.dot(a, b, precision=lax.Precision.HIGHEST, preferred_element_type=jnp.float32)

    grid = final_s[...]
    loads[2].wait()
    loads[3].wait()
    half3, half4 = dot(k_s[0], grid), dot(k_s[1], grid)
    grid, grid4 = dot(half3, l_s[0]), dot(half4, l_s[1])
    row = iota(grid.shape, 0)
    lane = iota(grid.shape, 1)
    inner_row = row % count
    gx, gy, gz = inner_row // cy, inner_row % cy, lane // step
    valid = lane % step < nz
    even3 = (gx % 2 == 0) & (gy % 2 == 0) & (gz % 2 == 0)
    even4 = (gx % 4 == 0) & (gy % 4 == 0) & (gz % 4 == 0)
    det3 = valid & ~even3
    det4 = valid & even3 & ~even4
    small3 = shrink(grid, thresh(FINE))
    small4 = shrink(grid4, thresh(FINE + 1))
    final_s[...] = jnp.where(even3, jnp.where(even4, grid4, small4), small3)

    def total(mask, v):
        return jnp.sum(jnp.sum(jnp.where(mask, v, 0.0), axis=0, keepdims=True), axis=1, keepdims=True)

    coarse = ((total(det3, grid * grid), total(det3, jnp.abs(small3))),
              (total(det4, grid4 * grid4), total(det4, jnp.abs(small4))))
    for q in (0, 1):
        line = jnp.zeros((1, LANES), jnp.float32)
        for level in range(LEVELS):
            weight = 8.0 ** (level + 1) / (7.0 * cells)
            if level < FINE:
                value = jnp.sum(jnp.where(one == 2 * level + q, tail, 0.0), axis=1, keepdims=True)
            else:
                value = coarse[level - FINE][q]
            line = jnp.where(one == level, value * weight, line)
        stats[q] = line[:, 0:LEVELS]

    first = pl.multiple_of((me[0] * ny + me[1]) * count, count)
    mine = pltpu.roll(final_s[pl.ds(first, count), :], lax.rem(LANES - me[2], LANES), 1)
    rows_s[...] = mine
    keep = iota((cy, LANES), 1) % step == 0
    for x in range(cx):
        spot = (0, step * x, pl.ds(0, cy, stride=step), slice(None))
        out[spot] = jnp.where(keep, rows_s[pl.ds(x * cy, cy), :], out[spot])


def shards(sizes, fields, exponents):
    nx, ny, nz = sizes
    ndev = nx * ny * nz
    _, lx, ly, lz = fields.shape
    cells = fields.size * ndev
    step = 2**FINE
    coarse = (lx // step, ly // step, lz // step)
    count = coarse[0] * coarse[1]
    tables = coarse_matrices(sizes, coarse)
    scratch = []
    for level in range(FINE):
        x, y = lx >> level, ly >> level
        scratch += [
            *(pltpu.VMEM(shape, jnp.float32) for shape in (
                (2, y, LANES), (2, y, LANES), (2, x, LANES), (2, x, LANES), (4, 1, LANES), (4, 1, LANES),
                (2, x, LANES), (y, LANES), (2, y, LANES), (y, LANES), (4, y, LANES), (2, 1, LANES),
                (4, 1, LANES), (2, 1, LANES), (8, 1, LANES), (x // 2, y, LANES), (x // 2, y // 2, LANES),
            )),
            pltpu.SemaphoreType.DMA((26,)),
            pltpu.SemaphoreType.DMA((26,)),
        ]
    height = -(-(count // 8 + 1) // 4) * 4
    scratch += [
        pltpu.VMEM((ndev, height, LANES), jnp.float32),
        pltpu.VMEM((height, LANES), jnp.float32),
        pltpu.VMEM((count, LANES), jnp.float32),
        pltpu.VMEM((nx * ny * count, LANES), jnp.float32),
        pltpu.SemaphoreType.DMA((ndev,)),
        pltpu.SemaphoreType.DMA((ndev,)),
        pltpu.VMEM(fields.shape, jnp.float32),
        pltpu.SMEM(exponents.shape, jnp.int32),
        pltpu.VMEM(tables[0].shape, jnp.float32),
        pltpu.VMEM(tables[1].shape, jnp.float32),
        pltpu.SemaphoreType.DMA((4,)),
    ]
    vmem = pl.BlockSpec(memory_space=pltpu.VMEM)
    return pl.pallas_call(
        functools.partial(kernel, sizes, cells),
        out_shape=(
            jax.ShapeDtypeStruct(fields.shape, jnp.float32),
            jax.ShapeDtypeStruct((2, 1, LEVELS), jnp.float32),
        ),
        in_specs=[pl.BlockSpec(memory_space=pltpu.HBM)] * 4,
        out_specs=(vmem, vmem),
        scratch_shapes=scratch,
        compiler_params=pltpu.CompilerParams(
            collective_id=0, has_side_effects=True, vmem_limit_bytes=VMEM_LIMIT
        ),
    )(exponents, fields, *tables)


def solution(mesh):
    sizes = tuple(mesh.shape[name] for name in ("gx", "gy", "gz"))
    placed = (P(None, "gx", "gy", "gz"), P())
    return jax.shard_map(
        functools.partial(shards, sizes),
        mesh=mesh,
        in_specs=placed,
        out_specs=placed,
        check_vma=False,
    )
```

```python
import functools

import numpy as np

import jax
import jax.numpy as jnp
from jax import lax
from jax.experimental import pallas as pl
from jax.experimental.pallas import tpu as pltpu
from jax.sharding import PartitionSpec as P

FINE = 3
LEVELS = 5
LANES = 128
BUFFERS = 19
VMEM_LIMIT = 67_043_328
MESH = pl.DeviceIdType.MESH


def periodic_lift(length):
    eye = np.eye(length)
    even, odd = eye[0::2], eye[1::2]
    detail = odd - 0.5 * (even + np.roll(even, -1, 0))
    smooth = even + 0.25 * (np.roll(detail, 1, 0) + detail)
    whole = np.zeros((length, length))
    whole[0::2] = smooth
    whole[1::2] = detail
    return whole


def second_lift(length):
    whole = np.zeros((length, length))
    whole[0::2, 0::2] = periodic_lift(length // 2)
    return whole


def coarse_matrices(sizes, coarse):
    nx, ny, nz = sizes
    cx, cy, cz = coarse
    rows = np.arange(nx * ny * cx * cy)
    dev, inner = rows // (cx * cy), rows % (cx * cy)
    gx = (dev // ny) * cx + inner // cy
    gy = (dev % ny) * cy + inner % cy
    step = LANES // cz
    lanes = np.array([z * step + d for d in range(nz) for z in range(cz)])
    result = []
    for both_levels in (False, True):
        mx, my, mz = periodic_lift(nx * cx), periodic_lift(ny * cy), periodic_lift(nz * cz)
        if both_levels:
            mx, my, mz = second_lift(nx * cx) @ mx, second_lift(ny * cy) @ my, second_lift(nz * cz) @ mz
        both = mx[gx[:, None], gx[None]] * my[gy[:, None], gy[None]]
        along = np.zeros((LANES, LANES))
        along[np.ix_(lanes, lanes)] = mz.T
        result.append((both.astype(np.float32), along.astype(np.float32)))
    return [np.stack(pair) for pair in zip(*result)]


def iota(shape, axis):
    return lax.broadcasted_iota(jnp.int32, shape, axis)


def roll(values, shift, axis):
    return pltpu.roll(values, shift % values.shape[axis], axis)


def lift_rows(v, low, high):
    n = v.shape[0]
    row = iota(v.shape, 0)
    odd = row % 2 == 1
    up = jnp.where(row == n - 1, high, roll(v, -1, 0))
    w = jnp.where(odd, v - 0.5 * (roll(v, 1, 0) + up), v)
    down = jnp.where(row == 0, low - 0.5 * v, roll(w, 1, 0))
    return jnp.where(odd, w, w + 0.25 * (down + roll(w, -1, 0)))


def lift_lanes(v, rim, s):
    lane = iota(v.shape, 1)
    up = jnp.where(lane == LANES - s, rim, roll(v, -s, 1))
    w = jnp.where(lane % (2 * s) == s, v - 0.5 * (roll(v, s, 1) + up), v)
    down = jnp.where(lane == 0, rim - 0.5 * v, roll(w, s, 1))
    return jnp.where(lane % (2 * s) == 0, w + 0.25 * (down + roll(w, -s, 1)), w)


def shrink(v, thresh):
    return v - jnp.clip(v, -thresh, thresh)


def kernel(sizes, cells, exps_in, field_in, rows_in, lanes_in, out, stats, *scratch):
    nx, ny, nz = sizes
    ndev = nx * ny * nz
    scratch = list(scratch)
    field, exps, k_s, l_s, in_sem = scratch[-5:]
    scratch = scratch[:-5]
    loads = [
        pltpu.make_async_copy(a, b, in_sem.at[i])
        for i, (a, b) in enumerate(((field_in, field), (exps_in, exps), (rows_in, k_s), (lanes_in, l_s)))
    ]
    for load in loads:
        load.start()
    me = (lax.axis_index("gx"), lax.axis_index("gy"), lax.axis_index("gz"))

    def device(dx, dy, dz):
        return (
            lax.rem(me[0] + (dx + nx), nx),
            lax.rem(me[1] + (dy + ny), ny),
            lax.rem(me[2] + (dz + nz), nz),
        )

    def thresh(level):
        return jnp.exp2(jnp.full((1, LANES), exps[level].astype(jnp.float32)))

    def split(j):
        return j // (ny * nz), (j // nz) % ny, j % nz

    barrier = pltpu.get_barrier_semaphore()

    near = max(sizes) // 2 <= FINE
    greeted = {
        tuple((d + size - 1) % size if near else d for d, size in zip(spot, sizes))
        for spot in np.ndindex(*(3, 3, 3) if near else sizes)
    } - {(0, 0, 0)}
    for spot in sorted(greeted):
        pl.semaphore_signal(barrier, inc=1, device_id=device(*spot), device_id_type=MESH)
    gath, msg, rows_s, final_s, g_send, g_recv = scratch[-6:]
    sums = []
    loads[0].wait()
    loads[1].wait()
    away = (-1, 1)
    alone = nx == 2

    for level in range(FINE):
        (xs, xr, ys, yr, es, er, yl, zs, zr, hs, hr, ds, dr, cs, cr, work, nxt, send_sem, recv_sem) = scratch[
            level * BUFFERS : level * BUFFERS + BUFFERS
        ]
        s = 2**level
        n = field.shape[2] // s
        px = field.shape[1] // s
        src = field.at[0] if level == 0 else scratch[(level - 1) * BUFFERS + 16]
        lane = iota((n, LANES), 1)

        def edge(v):
            return v[0:1], v[n - 1 : n] - 0.5 * v[n - 2 : n - 1]

        e_plane = src[0]
        p_plane = src[px - 1] - 0.5 * src[px - 2]
        xs[0] = e_plane
        xs[1] = p_plane
        ys[0] = src[:, 0, :]
        ys[1] = src[:, n - 1, :] - 0.5 * src[:, n - 2, :]
        for a, plane in ((0, e_plane), (1, p_plane)):
            es[2 * a], es[2 * a + 1] = edge(plane)

        packed = jnp.zeros((n, LANES), jnp.float32)
        for x in range(px):
            v = src[x]
            u = jnp.where(lane == LANES - s, v - 0.5 * roll(v, s, 1), v)
            at = 2 * s * x
            packed = jnp.where((lane == at) | (lane == at + s), roll(u, at + s, 1), packed)
        half = 2 * s * px
        combined = packed - 0.5 * roll(packed, 2 * s, 1)
        sides = roll(jnp.where(lane < half // 2, packed, combined), half, 1)
        zs[...] = packed
        hs[...] = sides
        ds[0], ds[1] = edge(packed)
        cs[0], cs[1] = edge(sides)

        if level == 0:
            pl.semaphore_wait(barrier, len(greeted))
        copies = []
        ways = (0,) if alone else (0, 1)
        for i in (0, 1):
            for b in (0, 1):
                for a in ways:
                    copies.append((cs.at[b], cr.at[4 * a + 2 * b + i], (away[a], away[b], away[i])))
                copies.append((ds.at[b], dr.at[2 * b + i], (0, away[b], away[i])))
        for a in (0, 1):
            for b in (0, 1):
                copies.append((es.at[2 * a + b], er.at[2 * a + b], (away[a], away[b], 0)))
        for b in (0, 1):
            copies.append((ys.at[b], yr.at[b], (0, away[b], 0)))
        for i in (0, 1):
            for a in ways:
                copies.append((hs, hr.at[2 * a + i], (away[a], 0, away[i])))
        for a in (0, 1):
            copies.append((xs.at[a], xr.at[a], (away[a], 0, 0)))
        for i in (0, 1):
            copies.append((zs, zr.at[i], (0, 0, away[i])))
        flights = [
            pltpu.make_async_remote_copy(
                src_ref=f, dst_ref=t, send_sem=send_sem.at[i], recv_sem=recv_sem.at[i],
                device_id=device(*d), device_id_type=MESH,
            )
            for i, (f, t, d) in enumerate(copies)
        ]
        for flight in flights:
            flight.start()
        if level > 0:
            sums += finish()
        for flight in flights:
            flight.wait()

        for b in (0, 1):
            yl[b] = lift_rows(yr[b], er[2 + b], er[b])

        def rim_of(main, side):
            spot = iota(main(0).shape, 1)
            parts = []
            for i in (0, 1):
                after = side(0, i)
                before = after if alone else side(1, i)
                v = jnp.where(spot < half, main(i), 0.0)
                v = jnp.where((spot >= half) & (spot < half + 2 * s), after, v)
                parts.append(jnp.where(spot >= LANES - 2 * s, before, v))
            v = jnp.where(spot % (2 * s) < s, roll(parts[0], -s, 1), roll(parts[1], s, 1))
            odd = (spot // (2 * s)) % 2 == 1
            w = jnp.where(odd, v - 0.5 * (roll(v, 2 * s, 1) + roll(v, -2 * s, 1)), v)
            return jnp.where(odd, w, w + 0.25 * (roll(w, 2 * s, 1) + roll(w, -2 * s, 1)))

        rim_rows = [
            rim_of(lambda i: dr[2 * b + i], lambda a, i: cr[4 * a + 2 * b + i]) for b in (0, 1)
        ]
        rim = rim_of(lambda i: zr[i], lambda a, i: hr[2 * a + i])
        rim = lift_rows(rim, rim_rows[1], rim_rows[0])
        level_thresh = thresh(level)
        inner = (lane % (2 * s) == 0) & (iota((n, LANES), 0) % 2 == 0)
        active = lane % s == 0

        def plane_step(x, v):
            v = lift_rows(v, yl[1, x : x + 1, :], yl[0, x : x + 1, :])
            v = lift_lanes(v, roll(rim, LANES - s - 2 * s * x, 1), s)
            work[x] = v
            if x % 2 == 0:
                nxt[x // 2] = work[x, pl.ds(0, n // 2, stride=2), :]

        def finish(level=level, work=work, px=px, n=n, s=s, inner=inner, active=active, t=level_thresh):
            energy = kept = jnp.zeros((n, LANES), jnp.float32)
            for x in range(px):
                v = work[x]
                small = shrink(v, t)
                use = active & ~inner if x % 2 == 0 else active
                energy += jnp.where(use, v * v, 0.0)
                kept += jnp.where(use, jnp.abs(small), 0.0)
                if level == 0:
                    out[0, x] = small
                else:
                    spot = (0, s * x, pl.ds(0, n, stride=s), slice(None))
                    out[spot] = jnp.where(active, small, out[spot])
            return [
                jnp.sum(jnp.sum(v, axis=0, keepdims=True), axis=1, keepdims=True) for v in (energy, kept)
            ]

        even = src[0]
        before = xr[1] - 0.5 * even
        for k in range(px // 2):
            after = src[2 * k + 2] if 2 * k + 2 < px else xr[0]
            detail = src[2 * k + 1] - 0.5 * (even + after)
            smooth = even + 0.25 * (before + detail)
            plane_step(2 * k, smooth)
            plane_step(2 * k + 1, detail)
            even, before = after, detail

    last = scratch[(FINE - 1) * BUFFERS + 16]
    cx, cy = last.shape[0], last.shape[1]
    step = 2**FINE
    count = cx * cy
    for x in range(cx):
        rows_s[pl.ds(x * cy, cy), :] = last[x]
    here = rows_s[...]
    lane = iota((count, LANES), 1)
    row = iota((count, LANES), 0)
    here = jnp.where(lane % step == 0, here, 0.0)
    for bit in (1, 2, 4):
        here = jnp.where((row & bit) != 0, roll(here, bit, 1), here)
    groups = count // 8
    one = iota((1, LANES), 1)
    for g in range(groups):
        msg[g : g + 1] = jnp.sum(here[8 * g : 8 * g + 8], axis=0, keepdims=True)
    tail = jnp.zeros((1, LANES), jnp.float32)
    for i, whole in enumerate(sums + finish()):
        tail = jnp.where(one == i, whole, tail)
    msg[groups:] = jnp.broadcast_to(tail, (msg.shape[0] - groups, LANES))
    flat = (me[0] * ny + me[1]) * nz + me[2]

    def post(j):
        return pltpu.make_async_remote_copy(
            src_ref=msg, dst_ref=gath.at[flat], send_sem=g_send.at[j], recv_sem=g_recv.at[j],
            device_id=device(*split(j)), device_id_type=MESH,
        )

    def send(j, carry):
        post(ndev - j).start()
        return carry

    def settle(j, carry):
        post(j).wait()
        return carry

    if ndev <= 32:
        posts = [post(ndev - j) for j in range(1, ndev)]
        for flight in posts:
            flight.start()
        gath[flat] = msg[...]
        for flight in posts:
            flight.wait()
    else:
        lax.fori_loop(1, ndev, send, 0)
        gath[flat] = msg[...]
        lax.fori_loop(1, ndev, settle, 0)

    sub = iota((8, LANES), 0)
    lane8 = iota((8, LANES), 1)

    def unpack(d, tail):
        for g in range(groups):
            acc = jnp.zeros((8, LANES), jnp.float32)
            for z in range(nz):
                v = jnp.broadcast_to(gath[d * nz + z, g : g + 1, :], (8, LANES))
                for bit in (1, 2, 4):
                    v = jnp.where((sub & bit) != 0, roll(v, -bit, 1), v)
                acc += roll(jnp.where(lane8 % step == 0, v, 0.0), z, 1)
            final_s[pl.ds(pl.multiple_of(d * count + 8 * g, 8), 8), :] = acc
        for z in range(nz):
            tail += gath[d * nz + z, groups : groups + 1, :]
        return tail

    tail = lax.fori_loop(0, nx * ny, unpack, jnp.zeros((1, LANES), jnp.float32), unroll=nx * ny <= 8)

    def dot(a, b):
        return jnp.dot(a, b, precision=lax.Precision.HIGHEST, preferred_element_type=jnp.float32)

    grid = final_s[...]
    loads[2].wait()
    loads[3].wait()
    half3, half4 = dot(k_s[0], grid), dot(k_s[1], grid)
    grid, grid4 = dot(half3, l_s[0]), dot(half4, l_s[1])
    row = iota(grid.shape, 0)
    lane = iota(grid.shape, 1)
    inner_row = row % count
    gx, gy, gz = inner_row // cy, inner_row % cy, lane // step
    valid = lane % step < nz
    even3 = (gx % 2 == 0) & (gy % 2 == 0) & (gz % 2 == 0)
    even4 = (gx % 4 == 0) & (gy % 4 == 0) & (gz % 4 == 0)
    det3 = valid & ~even3
    det4 = valid & even3 & ~even4
    small3 = shrink(grid, thresh(FINE))
    small4 = shrink(grid4, thresh(FINE + 1))
    final_s[...] = jnp.where(even3, jnp.where(even4, grid4, small4), small3)

    def total(mask, v):
        return jnp.sum(jnp.sum(jnp.where(mask, v, 0.0), axis=0, keepdims=True), axis=1, keepdims=True)

    coarse = ((total(det3, grid * grid), total(det3, jnp.abs(small3))),
              (total(det4, grid4 * grid4), total(det4, jnp.abs(small4))))
    for q in (0, 1):
        line = jnp.zeros((1, LANES), jnp.float32)
        for level in range(LEVELS):
            weight = 8.0 ** (level + 1) / (7.0 * cells)
            if level < FINE:
                value = jnp.sum(jnp.where(one == 2 * level + q, tail, 0.0), axis=1, keepdims=True)
            else:
                value = coarse[level - FINE][q]
            line = jnp.where(one == level, value * weight, line)
        stats[q] = line[:, 0:LEVELS]

    first = pl.multiple_of((me[0] * ny + me[1]) * count, count)
    mine = pltpu.roll(final_s[pl.ds(first, count), :], lax.rem(LANES - me[2], LANES), 1)
    rows_s[...] = mine
    keep = iota((cy, LANES), 1) % step == 0
    for x in range(cx):
        spot = (0, step * x, pl.ds(0, cy, stride=step), slice(None))
        out[spot] = jnp.where(keep, rows_s[pl.ds(x * cy, cy), :], out[spot])


def shards(sizes, fields, exponents):
    nx, ny, nz = sizes
    ndev = nx * ny * nz
    _, lx, ly, lz = fields.shape
    cells = fields.size * ndev
    step = 2**FINE
    coarse = (lx // step, ly // step, lz // step)
    count = coarse[0] * coarse[1]
    tables = coarse_matrices(sizes, coarse)
    scratch = []
    for level in range(FINE):
        x, y = lx >> level, ly >> level
        scratch += [
            *(pltpu.VMEM(shape, jnp.float32) for shape in (
                (2, y, LANES), (2, y, LANES), (2, x, LANES), (2, x, LANES), (4, 1, LANES), (4, 1, LANES),
                (2, x, LANES), (y, LANES), (2, y, LANES), (y, LANES), (4, y, LANES), (2, 1, LANES),
                (4, 1, LANES), (2, 1, LANES), (8, 1, LANES), (x, y, LANES), (x // 2, y // 2, LANES),
            )),
            pltpu.SemaphoreType.DMA((26,)),
            pltpu.SemaphoreType.DMA((26,)),
        ]
    height = -(-(count // 8 + 1) // 4) * 4
    scratch += [
        pltpu.VMEM((ndev, height, LANES), jnp.float32),
        pltpu.VMEM((height, LANES), jnp.float32),
        pltpu.VMEM((count, LANES), jnp.float32),
        pltpu.VMEM((nx * ny * count, LANES), jnp.float32),
        pltpu.SemaphoreType.DMA((ndev,)),
        pltpu.SemaphoreType.DMA((ndev,)),
        pltpu.VMEM(fields.shape, jnp.float32),
        pltpu.SMEM(exponents.shape, jnp.int32),
        pltpu.VMEM(tables[0].shape, jnp.float32),
        pltpu.VMEM(tables[1].shape, jnp.float32),
        pltpu.SemaphoreType.DMA((4,)),
    ]
    vmem = pl.BlockSpec(memory_space=pltpu.VMEM)
    return pl.pallas_call(
        functools.partial(kernel, sizes, cells),
        out_shape=(
            jax.ShapeDtypeStruct(fields.shape, jnp.float32),
            jax.ShapeDtypeStruct((2, 1, LEVELS), jnp.float32),
        ),
        in_specs=[pl.BlockSpec(memory_space=pltpu.HBM)] * 4,
        out_specs=(vmem, vmem),
        scratch_shapes=scratch,
        compiler_params=pltpu.CompilerParams(
            collective_id=0, has_side_effects=True, vmem_limit_bytes=VMEM_LIMIT
        ),
    )(exponents, fields, *tables)


def solution(mesh):
    sizes = tuple(mesh.shape[name] for name in ("gx", "gy", "gz"))
    placed = (P(None, "gx", "gy", "gz"), P())
    return jax.shard_map(
        functools.partial(shards, sizes),
        mesh=mesh,
        in_specs=placed,
        out_specs=placed,
        check_vma=False,
    )
```
